32 devices in a mesh: row: 8 (over y, x, core), col: 4 (over z).
Axes of the slice: x: 2, y: 2, z: 4, core: 2. Of those that a mesh axis runs over, the one named last changes fastest.
Arguments:
- integrals: bfloat16 [320, 32, 4096], P('row', None, 'col'), may hold values from -6 to 6
- coeffs: bfloat16 [10240, 4096], P('row', 'col'), may hold values from -0.078125 to 0.078125
- mask: int32 [320, 4], replicated, may hold values from 0 to 1, as said below
- offsets: int32 [321], replicated, may hold values from 0 to 7680, as said below
- atom_of_slot: int32 [320], replicated, may hold values from 0 to 319, as said below
Outputs:
- half_transformed: bfloat16 [4096, 4096], P('row', 'col')
The draws below stay inside these ranges and needn't reach their ends.
Inputs may be any that keep to these rules, and one draw needn't show every extreme that they name: `mask`: 1 marks a significant pair of an atom and a block of 64 window functions. offsets[0] = 0 and offsets[a + 1] - offsets[a] is atom a's number of basis functions, 16 to 32; atoms 2k and 2k + 1 together have 3 * 16; rows of an atom's padded block past its number are padding. `atom_of_slot`: a permutation of the atoms; slot k is held by atom owner k // 40 along row, and atom a's AO-row owner is a // 40; one atom owner holds at least one and at most 5 atoms of any one AO-row owner, and exactly 5 for some pairs.
All inputs are finite; a program needn't handle non-finite values.
Results may differ from the reference program's by a relative error of at most 0.015.
Values may be sent and summed in bfloat16 or wider, within the bound.
A program may use at most 256 MiB of HBM per device.

```python
import jax
import jax.numpy as jnp
from jax import lax

AW = 32
ATOMS_DEV = 40
NOCC = 4096
NAUX = 16
NU_DEV = 64
NATOM = 320
NBAS = 10240
NU = 256
NVB = 4
CAP = 5
N_ROW = 8


def draw_mask(key, part):
    first_key = jax.random.fold_in(key, 11)
    second_key = jax.random.fold_in(key, 12)
    percent = jax.random.randint(first_key, (N_ROW,), 10, 96)
    rolled = jax.random.randint(second_key, (NATOM, NVB), 0, 100)
    owner = jnp.arange(NATOM, dtype=jnp.int32) // ATOMS_DEV
    return (rolled < percent[owner][:, None]).astype(jnp.int32)


def draw_offsets(key, part):
    firsts = jax.random.randint(jax.random.fold_in(key, 21), (NATOM // 2,), AW // 2, AW + 1)
    seconds = 3 * AW // 2 - firsts
    counts = jnp.stack([firsts, seconds], axis=1).reshape(-1).astype(jnp.int32)
    return jnp.concatenate([jnp.zeros((1,), jnp.int32), jnp.cumsum(counts).astype(jnp.int32)])


def draw_atom_of_slot(key, part):
    first_key = jax.random.fold_in(key, 31)
    second_key = jax.random.fold_in(key, 32)
    third_key = jax.random.fold_in(key, 33)
    fourth_key = jax.random.fold_in(key, 34)
    every_shift = jax.random.permutation(first_key, jnp.arange(N_ROW, dtype=jnp.int32))
    repeated = jnp.tile(jnp.arange(N_ROW, dtype=jnp.int32), CAP - 1)
    extra = jax.random.permutation(third_key, repeated)[:ATOMS_DEV - N_ROW]
    shifts = jax.random.permutation(fourth_key, jnp.concatenate([every_shift, extra]).astype(jnp.int32))
    locals_table = jax.vmap(lambda owner: jax.random.permutation(jax.random.fold_in(second_key, owner), ATOMS_DEV))(jnp.arange(N_ROW, dtype=jnp.int32))
    source = jnp.arange(N_ROW, dtype=jnp.int32)[:, None]
    layer = jnp.arange(ATOMS_DEV, dtype=jnp.int32)[None, :]
    target = (source - shifts[None, :]) % N_ROW
    chosen = locals_table[target, jnp.broadcast_to(layer, target.shape)].astype(jnp.int32)
    return (target * ATOMS_DEV + chosen).reshape(-1).astype(jnp.int32)


def strengthened(drawn, stream_key, source, target, parts, factor):
    def block_of(axis_at):
        return (jnp.arange(drawn.shape[axis_at]) // (drawn.shape[axis_at] // parts)).reshape((-1,) + (1,) * (drawn.ndim - 1 - axis_at))

    one_side = jax.random.permutation(stream_key, parts)[block_of(target)]
    second = (block_of(target) + parts // 2) % parts
    return jnp.where((block_of(source) == one_side) | (block_of(source) == second), factor * drawn, drawn)


def block_levels(rng, dims, split, smallest, largest):
    level = 1.0
    for position, shards_of in split:
        steps = jax.random.uniform(jax.random.fold_in(jax.random.fold_in(rng, 6), position), (shards_of,), jnp.float32, smallest / len(split), largest / len(split))
        level = level * jnp.repeat(jnp.exp(steps), dims[position] // shards_of).reshape((-1,) + (1,) * (len(dims) - 1 - position))
    return level


def normal_values(own_key, extent, spread, bound, shards=(), kind=jnp.bfloat16):
    result = spread * jax.random.normal(own_key, extent, jnp.float32)
    if shards:
        result = result * block_levels(own_key, extent, shards, -0.22, 0.18)
    return jnp.clip(result, -bound, bound).astype(kind)


def gaussian_with(rng, dims, scale, reach, cuts, heavy, held_as=jnp.bfloat16):
    drawn = scale * jax.random.normal(rng, dims, jnp.float32)
    if cuts:
        drawn = drawn * block_levels(rng, dims, cuts, -0.22, 0.18)
    return jnp.clip(strengthened(drawn, jax.random.fold_in(rng, 3), *heavy), -reach, reach).astype(held_as)


def setup_inputs(seed: int = 0) -> dict:
    key_list = jax.random.split(jax.random.key(seed), 6)
    return {
        "integrals": normal_values(key_list[0], (NATOM, AW, NU * NAUX), 1.0, 6.0, ((0, 8), (2, 4))),
        "coeffs": gaussian_with(key_list[1], (NBAS, NOCC), NBAS ** -0.5, 0.078125, ((0, 8), (1, 4)), (0, 1, 8, 2.0)),
        "mask": draw_mask(jax.random.fold_in(key_list[5], 71), 0),
        "offsets": draw_offsets(jax.random.fold_in(key_list[5], 71), 0),
        "atom_of_slot": draw_atom_of_slot(jax.random.fold_in(key_list[5], 71), 0),
    }


def reference(integrals, coeffs, mask, offsets, atom_of_slot):
    natoms = integrals.shape[0]
    inverse = jnp.zeros((natoms,), jnp.int32).at[atom_of_slot].set(jnp.arange(natoms, dtype=jnp.int32))
    ordered = integrals[inverse]
    lengths = offsets[1:] - offsets[:-1]
    row_live = (jnp.arange(AW, dtype=jnp.int32)[None, :] < lengths[:, None]).astype(jnp.bfloat16)
    column_live = jnp.repeat(mask, NU_DEV * NAUX, axis=1).astype(jnp.bfloat16)
    kept = ordered * row_live[:, :, None] * column_live[:, None, :]
    width = kept.shape[2]
    kept_groups = kept.reshape(N_ROW, ATOMS_DEV * AW, width)
    coeff_groups = coeffs.reshape(N_ROW, ATOMS_DEV * AW, coeffs.shape[1])

    def add_owner(total, pieces):
        coeff_piece, kept_piece = pieces
        part = lax.dot_general(coeff_piece, kept_piece, (((0,), (0,)), ((), ())), preferred_element_type=jnp.float32)
        part = lax.optimization_barrier(part.astype(jnp.bfloat16))
        return total + part.astype(jnp.float32), None

    start = jnp.zeros((coeffs.shape[1], width), jnp.float32)
    half, unused = lax.scan(add_owner, start, (coeff_groups, kept_groups))
    return half.astype(jnp.bfloat16)
```

```python
import functools

import jax
import jax.numpy as jnp
from jax import lax
from jax.experimental import pallas as pl
from jax.experimental.pallas import tpu as pltpu
from jax.sharding import PartitionSpec as P

MESH = pl.DeviceIdType.MESH
F32 = jnp.float32
BF16 = jnp.bfloat16
LANES = 128
EARLY = 2
PIECES = 4
HALVES = 2
JOIN = 2
LAG = 4
PASS_LAG = 2


def remote(src, dst, send, recv, device):
    return pltpu.make_async_remote_copy(
        src_ref=src, dst_ref=dst, send_sem=send, recv_sem=recv, device_id=device, device_id_type=MESH
    )


def nearest(me, n, s):
    m = jnp.minimum(me, n - 1 - me)
    step = (s + 1) // 2
    near = jnp.where(s % 2 == 1, me - step, me + step)
    far = jnp.where(me <= n - 1 - me, s, n - 1 - s)
    return jnp.where(s <= 2 * m, near, far)


def kernel(n_row, n_col, cap, n_chunk, *refs):
    meta, offsets, weight, integrals, coeffs, out = refs[:6]
    asend, arecv = refs[6 : 6 + PIECES], refs[6 + PIECES : 6 + 2 * PIECES]
    (
        kept, kept_end, gathered, work, core_in, work_far, core_far, pair, sums,
        a_ss, a_rs, r_ss, l_ss, g_rs, c_ss, c_rs, d_ss, d_rs, p_ss, p_rs, t_ss, t_rs, f_ss, f_rs, k_ss, k_rs,
    ) = refs[6 + 2 * PIECES :]
    me = lax.axis_index("row")
    plane = lax.axis_index("col")
    core = me % 2
    chip = me // 2
    n_chip = n_row // 2
    partner = me + 1 - 2 * core
    buddy = chip + 1 - 2 * (chip % 2)
    per_dev, atom_w, row_width = integrals.shape
    half = atom_w // 2
    pairs = per_dev // 2
    packed = 3 * half
    slots = n_row * cap
    per_plane = n_row // n_col
    chips_plane = per_plane // 2
    n_kb = n_chunk // per_plane
    piece = row_width // PIECES
    half_width = row_width // HALVES
    per_half = PIECES // HALVES
    n_far = n_col - 2
    inner = n_col - 2
    has_left = plane > 0
    has_right = plane < n_col - 1
    is_end = (plane == 0) | (plane == n_col - 1)
    is_helper = (plane == 1) | (plane == n_col - 2)
    low_half = plane <= n_col - 1 - plane
    near_end = jnp.where(low_half, 0, n_col - 1)
    far_end = n_col - 1 - near_end
    helper_plane = jnp.where(low_half, 1, n_col - 2)

    barrier = pltpu.get_barrier_semaphore()
    for other in range(1, n_row):
        pl.semaphore_signal(barrier, inc=1, device_id=((me + other) % n_row, plane), device_id_type=MESH)

    @pl.when(has_left)
    def _():
        pl.semaphore_signal(barrier, inc=1, device_id=(me, plane - 1), device_id_type=MESH)

    @pl.when(has_right)
    def _():
        pl.semaphore_signal(barrier, inc=1, device_id=(me, plane + 1), device_id_type=MESH)

    def selection(p, weighted):
        s = lax.broadcasted_iota(jnp.int32, (packed, 2 * atom_w), 0)
        t = lax.broadcasted_iota(jnp.int32, (packed, 2 * atom_w), 1)
        first = me * per_dev + 2 * p
        extra = offsets[first + 1] - offsets[first] - half
        source = jnp.where(
            s < half, s, jnp.where(s < 2 * half, s + half, jnp.where(s - 2 * half < extra, s - half, s + half - extra))
        )
        hit = source == t
        if weighted:
            sig = jnp.where(t < atom_w, weight[first], weight[first + 1])
            hit = hit & (sig > 0)
        return jnp.where(hit, 1.0, 0.0).astype(BF16)

    def column(n):
        return ((n % per_plane) * n_kb + n // per_plane) * LANES

    def pack_coeffs(chunks):
        def pack(p, carry):
            at = pl.ds(pl.multiple_of(p * packed, 16), packed)
            rows = pl.ds(pl.multiple_of(p * 2 * atom_w, 2 * atom_w), 2 * atom_w)
            pick = selection(p, False)
            live = jnp.concatenate([coeffs[rows, column(n) : column(n) + LANES] for n in chunks], axis=1)
            live = jnp.dot(pick, live, preferred_element_type=F32).astype(BF16)
            for i, n in enumerate(chunks):
                gathered[plane, n, at, :] = live[:, i * LANES : (i + 1) * LANES]
            return carry

        lax.fori_loop(0, pairs, pack, 0, unroll=4)

    def to_right(z, n):
        return remote(gathered.at[z, n], gathered.at[z, n], r_ss.at[z, n], g_rs.at[z, n], (me, plane + 1))

    def to_left(z, n):
        return remote(gathered.at[z, n], gathered.at[z, n], l_ss.at[z, n], g_rs.at[z, n], (me, plane - 1))

    def goes_right(z):
        return (z <= plane) & has_right & ((plane != n_col - 2) | (z == plane))

    def goes_left(z):
        return (z >= plane) & has_left & ((plane != 1) | (z == plane))

    def forward(z, n):
        @pl.when(goes_right(z))
        def _():
            to_right(z, n).start()

        @pl.when(goes_left(z))
        def _():
            to_left(z, n).start()

    early = min(EARLY, n_chunk)
    pack_coeffs(range(early))
    pl.semaphore_wait(barrier, n_row - 1 + has_left.astype(jnp.int32) + has_right.astype(jnp.int32))
    for n in range(early):
        forward(plane, n)

    def a_copy(q, owner):
        return remote(asend[q].at[owner], arecv[q].at[me], a_ss.at[q, owner], a_rs.at[q, me], (owner, plane))

    for q in range(PIECES):
        lanes = slice(q * piece, (q + 1) * piece)

        def place(step, carry):
            owner = (me + step) % n_row

            @pl.when(step > 0)
            def _():
                for c in range(cap):
                    asend[q][owner, c] = integrals[meta[owner * cap + c], :, lanes]
                a_copy(q, owner).start()

            @pl.when(step == 0)
            def _():
                for c in range(cap):
                    arecv[q][me, c] = integrals[meta[me * cap + c], :, lanes]

            return carry

        lax.fori_loop(0, n_row, place, 0)

    if early < n_chunk:
        pack_coeffs(range(early, n_chunk))

        @pl.when(jnp.logical_not(is_end))
        def _():
            for n in range(early, n_chunk):
                forward(plane, n)

    def kept_copy(q):
        lanes, there = pl.ds(q * piece, piece), pl.ds(q % per_half * piece, piece)
        return remote(
            kept.at[:, lanes], kept_end.at[q // per_half, :, there], k_ss.at[q], k_rs.at[q], (me, helper_plane)
        )

    for q in range(PIECES):
        lanes = slice(q * piece, (q + 1) * piece)

        def wait_blocks(step, carry):
            source = (me + step) % n_row
            remote(
                asend[q].at[source], arecv[q].at[source], a_ss.at[q, source], a_rs.at[q, source], (source, plane)
            ).wait_recv()
            return carry

        lax.fori_loop(1, n_row, wait_blocks, 0)

        def pack_kept(p, carry):
            first, second = meta[slots + 2 * p], meta[slots + 2 * p + 1]
            rows = jnp.concatenate(
                [arecv[q][first // cap, first % cap], arecv[q][second // cap, second % cap]], axis=0
            )
            live = jnp.dot(selection(p, True), rows, preferred_element_type=F32).astype(BF16)
            kept[pl.ds(pl.multiple_of(p * packed, 16), packed), lanes] = live
            return carry

        lax.fori_loop(0, pairs, pack_kept, 0, unroll=4)

        @pl.when(is_end)
        def _():
            kept_copy(q).start()

    def kept_copy_in(h, i):
        q, there = h * per_half + i, pl.ds(i * piece, piece)
        return remote(
            kept.at[:, there], kept_end.at[h, :, there], k_ss.at[q], k_rs.at[q], (me, helper_plane)
        )

    @pl.when(is_end)
    def _():
        for n in range(early, n_chunk):
            forward(plane, n)

    def arrive(z, n):
        to_right(z, n).wait_recv()
        forward(z, n)

    @pl.when(jnp.logical_not(is_end))
    def _():
        for n in range(early):
            arrive(near_end, n)

    inside = inner * (n_chunk // 2)
    per_pass = (n_far - 1) * (n_chunk // 2)
    one = inside + per_pass
    two = one + early // 2
    three = two + (HALVES - 1) * per_pass
    group = 2 + HALVES
    steps = jnp.where(is_end, n_chunk, three + group * n_chunk)
    beside = jnp.where(low_half, 1, n_col - 2)

    def far_plane(f):
        return jnp.where(low_half, f + 2, n_col - 3 - f)

    def decode(s):
        first = s < inside
        last = s >= three
        near_wide = (s >= one) & (s < two)
        far_wide = jnp.logical_not(first | last | near_wide)
        v = jnp.where(s < one, s - inside, s - two + per_pass)
        u = s - three
        m, r = u // group + 1, u % group
        near = last & (r == 0)
        far_single = last & (r > 0) & (r <= HALVES)
        far = (far_wide | far_single) & jnp.logical_not(is_end)
        z = jnp.where(
            first, 1 + nearest(plane - 1, inner, s % inner), jnp.where(near_wide | near, near_end, far_end)
        )
        n = jnp.where(
            first,
            s // inner * 2,
            jnp.where(near_wide, (s - one) * 2, jnp.where(far_wide, v % (n_chunk // 2) * 2, jnp.where(near, m, m - 1))),
        )
        f = jnp.where(far_wide, v % per_pass // (n_chunk // 2), n_far - 1)
        h = jnp.where(far_wide, v // per_pass, r - 1)
        z = jnp.where(far, far_plane(f), z)
        late = last & (n < n_chunk) & (jnp.logical_not(near) | (n >= early))
        valid = first | near_wide | (far_wide & is_helper) | (late & (is_helper | jnp.logical_not(far_single)))
        comes = (first & (z != plane)) | (late & (r <= 1))
        z = jnp.where(is_end, jnp.where(s % 2 == 0, plane, beside), z)
        n = jnp.where(is_end, s // 2 * 2, n)
        comes = jnp.where(is_end, s % 2 == 1, comes)
        wide = jnp.logical_not(last) | is_end
        running = (s >= 0) & (s < steps)
        valid = (valid | is_end) & running
        n = jnp.clip(n, 0, n_chunk - 1)
        h = jnp.clip(h, 0, HALVES - 1)
        return valid & jnp.logical_not(far), valid & far, comes & running, wide, z, n, f, h

    def mine(wide, n):
        return wide | (n % 2 == core), jnp.where(wide, n + core, n)

    def other(wide, n):
        return wide | (n % 2 != core), jnp.where(wide, n + 1 - core, n)

    def core_copy(z, n):
        return remote(work.at[z, n], core_in.at[z, n // 2], c_ss.at[z, n], c_rs.at[z, n // 2], (partner, plane))

    def far_core_copy(f, n, h):
        return remote(
            work_far.at[f, n, h], core_far.at[f, n // 2, h], d_ss.at[f, n, h], d_rs.at[f, n // 2, h], (partner, plane)
        )

    def far_copy(f, z, n, h, to):
        lanes = pl.ds(pl.multiple_of(h * half_width, LANES), half_width)
        return remote(work_far.at[f, n, h], work.at[z, n, :, lanes], f_ss.at[f, n, h], f_rs.at[f, n, h], (me, to))

    def target(z, n):
        return z * chips_plane + (n % per_plane) // 2

    def half_lanes(h):
        return pl.ds(pl.multiple_of(h * half_width, LANES), half_width)

    def pair_copy(z, n, h):
        return remote(
            work.at[z, n, :, half_lanes(h)], pair.at[z, n // 2, :, half_lanes(h)], p_ss.at[z, n, h],
            p_rs.at[z, n // 2, h], (2 * buddy + core, plane),
        )

    def target_copy(z, n, h):
        return remote(
            work.at[z, n, :, half_lanes(h)], sums.at[chip // 2, n // per_plane, :, half_lanes(h)], t_ss.at[z, n, h],
            t_rs.at[chip // 2, n // per_plane, h], (2 * target(z, n) + core, plane),
        )

    def sends_pair(z, n):
        return target(z, n) % 2 != chip % 2

    def sends_sum(z, n):
        return (target(z, n) % 2 == chip % 2) & (target(z, n) != chip)

    def multiply(lhs, rhs):
        return lax.dot_general(lhs, rhs, (((0,), (0,)), ((), ())), preferred_element_type=F32).astype(BF16)

    def add(x, y):
        return (x.astype(F32) + y.astype(F32)).astype(BF16)

    def compute(s):
        own, far, comes, wide, z, n, f, h = decode(s)

        @pl.when(comes)
        def _():
            arrive(z, n)

            @pl.when(wide)
            def _():
                arrive(z, n + 1)

        def both():
            return jnp.concatenate([gathered[z, n], gathered[z, n + 1]], axis=1)

        @pl.when(own & wide)
        def _():
            part = multiply(both(), kept[...])
            work[z, n] = part[:LANES]
            work[z, n + 1] = part[LANES:]

        @pl.when(own & jnp.logical_not(wide))
        def _():
            work[z, n] = multiply(gathered[z, n], kept[...])

        @pl.when(far & wide)
        def _():
            @pl.when((f == 0) & (n == 0))
            def _():
                for i in range(per_half):
                    kept_copy_in(h, i).wait_recv()

            part = multiply(both(), kept_end[h])
            work_far[f, n, h] = part[:LANES]
            work_far[f, n + 1, h] = part[LANES:]

        @pl.when(far & jnp.logical_not(wide))
        def _():
            work_far[f, n, h] = multiply(gathered[z, n], kept_end[h])

        there, n_other = other(wide, n)

        @pl.when(own & there)
        def _():
            core_copy(z, n_other).start()

        @pl.when(far & there)
        def _():
            far_core_copy(f, n_other, h).start()

    def join_cores(s):
        own, far, comes, wide, z, n, f, h = decode(s)
        here, n = mine(wide, n)

        @pl.when(own & here)
        def _():
            core_copy(z, n).wait_recv()
            work[z, n] = add(work[z, n], core_in[z, n // 2])

            @pl.when(sends_pair(z, n))
            def _():
                for i in range(HALVES):
                    pair_copy(z, n, i).start()

        @pl.when(far & here)
        def _():
            far_core_copy(f, n, h).wait_recv()
            work_far[f, n, h] = add(work_far[f, n, h], core_far[f, n // 2, h])
            far_copy(f, z, n, h, near_end).start()

    def join_chips(s, carry):
        own, far, comes, wide, z, n, f, h = decode(s)
        here, n = mine(wide, n)

        @pl.when(own & here & sends_sum(z, n))
        def _():
            for i in range(HALVES):
                pair_copy(z, n, i).wait_recv()
            work[z, n] = add(work[z, n], pair[z, n // 2])
            for i in range(HALVES):
                target_copy(z, n, i).start()

        return carry

    def joined(s):
        return jnp.clip(jnp.minimum(2 * (s - three + 1), s - LAG), 0, steps)

    def step_body(s, carry):
        compute(s)
        join_cores(s - JOIN)
        lax.fori_loop(joined(s - 1), joined(s), join_chips, 0)
        return carry

    lax.fori_loop(0, steps + JOIN, step_body, 0)
    lax.fori_loop(joined(steps + JOIN - 1), steps, join_chips, 0)

    n_pass = n_far * n_chunk * HALVES

    def passed(e):
        v = e % ((n_far - 1) * n_chunk)
        w = e - (n_far - 1) * n_chunk * HALVES
        f = jnp.where(w < 0, v // n_chunk, n_far - 1)
        n = jnp.where(w < 0, v % n_chunk, w // HALVES)
        h = jnp.where(w < 0, e // ((n_far - 1) * n_chunk), w % HALVES)
        return f, far_plane(f), n, h

    @pl.when(is_end)
    def _():
        def pass_on(e, carry):
            @pl.when(e < n_pass)
            def _():
                f, z, n, h = passed(e)

                @pl.when(n % 2 == core)
                def _():
                    far_copy(f, z, n, h, plane).wait_recv()

                    @pl.when(sends_pair(z, n))
                    def _():
                        pair_copy(z, n, h).start()

            @pl.when(e >= PASS_LAG)
            def _():
                f, z, n, h = passed(e - PASS_LAG)

                @pl.when((n % 2 == core) & sends_sum(z, n))
                def _():
                    pair_copy(z, n, h).wait_recv()
                    lanes = half_lanes(h)
                    work[z, n, :, lanes] = add(work[z, n, :, lanes], pair[z, n // 2, :, lanes])
                    target_copy(z, n, h).start()

            return carry

        lax.fori_loop(0, n_pass + PASS_LAG, pass_on, 0)

    own_z, own_b = me // per_plane, me % per_plane
    for kb in range(n_kb):
        n = kb * per_plane + own_b
        for h in range(HALVES):
            pair_copy(own_z, n, h).wait_recv()
        total = work[own_z, n].astype(F32) + pair[own_z, n // 2].astype(F32)
        for step in range(1, n_chip // 2):
            source = (chip // 2 + step) % (n_chip // 2)
            for h in range(HALVES):
                remote(
                    work.at[own_z, n, :, half_lanes(h)], sums.at[source, kb, :, half_lanes(h)], t_ss.at[own_z, n, h],
                    t_rs.at[source, kb, h], (2 * (2 * source + chip % 2) + core, plane),
                ).wait_recv()
            total += sums[source, kb].astype(F32)
        out[kb * LANES : (kb + 1) * LANES, :] = total.astype(BF16)

    def drain_blocks(step, carry):
        for q in range(PIECES):
            a_copy(q, (me + step) % n_row).wait_send()
        return carry

    lax.fori_loop(1, n_row, drain_blocks, 0)

    def drain_sums(z, n, h):
        @pl.when(sends_pair(z, n))
        def _():
            pair_copy(z, n, h).wait_send()

        @pl.when(sends_sum(z, n))
        def _():
            target_copy(z, n, h).wait_send()

    def drain(s, carry):
        own, far, comes, wide, z, n, f, h = decode(s)
        here, n_mine = mine(wide, n)
        there, n_other = other(wide, n)

        @pl.when(own & there)
        def _():
            core_copy(z, n_other).wait_send()

        @pl.when(far & there)
        def _():
            far_core_copy(f, n_other, h).wait_send()

        @pl.when(far & here)
        def _():
            far_copy(f, z, n_mine, h, near_end).wait_send()

        @pl.when(own & here)
        def _():
            for i in range(HALVES):
                drain_sums(z, n_mine, i)

        return carry

    lax.fori_loop(0, steps, drain, 0)

    def drain_gathered(e, carry):
        z, n = e // n_chunk, e % n_chunk

        @pl.when(goes_right(z))
        def _():
            to_right(z, n).wait_send()

        @pl.when(goes_left(z))
        def _():
            to_left(z, n).wait_send()

        return carry

    lax.fori_loop(0, n_col * n_chunk, drain_gathered, 0)

    @pl.when(is_end)
    def _():
        for q in range(PIECES):
            kept_copy(q).wait_send()

        def drain_pass(e, carry):
            f, z, n, h = passed(e)

            @pl.when(n % 2 == core)
            def _():
                drain_sums(z, n, h)

            return carry

        lax.fori_loop(0, n_pass, drain_pass, 0)


def body(integrals, coeffs, mask, offsets, atom_of_slot):
    n_row = lax.axis_size("row")
    n_col = lax.axis_size("col")
    me = lax.axis_index("row")
    per_dev, atom_w, row_width = integrals.shape
    rows, cols = coeffs.shape
    cap = max(2, -(-per_dev // n_row))
    slots = n_row * cap
    n_atom = atom_of_slot.shape[0]
    block = cols * n_col // n_row
    n_chunk = cols // LANES
    n_kb = block // LANES

    slot = jnp.arange(n_atom, dtype=jnp.int32)
    owner = atom_of_slot // per_dev
    holder = slot // per_dev
    flow = holder * n_row + owner
    rank = jnp.sum(((flow[None, :] == flow[:, None]) & (slot[None, :] < slot[:, None])).astype(jnp.int32), axis=1)
    goes = jnp.where(holder == me, owner * cap + rank, -1)
    comes = atom_of_slot - me * per_dev + slots
    entry = jnp.arange(slots + per_dev, dtype=jnp.int32)[:, None]
    meta = jnp.sum(
        jnp.where(
            entry < slots,
            jnp.where(goes[None, :] == entry, (slot - me * per_dev)[None, :], 0),
            jnp.where(comes[None, :] == entry, (holder * cap + rank)[None, :], 0),
        ),
        axis=1,
    )

    column = jnp.arange(n_col, dtype=jnp.int32)[None, :] == lax.axis_index("col")
    weight = jnp.sum(jnp.where(column, mask, 0), axis=1)

    packed = rows * 3 // 4
    dma = pltpu.SemaphoreType.DMA
    n_chip = n_row // 2
    n_far = n_col - 2
    narrow = row_width // HALVES
    moved = [pltpu.VMEM((n_row, cap, atom_w, row_width // PIECES), BF16)] * (2 * PIECES)
    smem = pl.BlockSpec(memory_space=pltpu.SMEM)
    vmem = pl.BlockSpec(memory_space=pltpu.VMEM)
    return pl.pallas_call(
        functools.partial(kernel, n_row, n_col, cap, n_chunk),
        out_shape=jax.ShapeDtypeStruct((block, row_width), BF16),
        in_specs=[smem, smem, smem, vmem, vmem],
        out_specs=vmem,
        scratch_shapes=moved
        + [
            pltpu.VMEM((packed, row_width), BF16),
            pltpu.VMEM((HALVES, packed, narrow), BF16),
            pltpu.VMEM((n_col, n_chunk, packed, LANES), BF16),
            pltpu.VMEM((n_col, n_chunk, LANES, row_width), BF16),
            pltpu.VMEM((n_col, n_chunk // 2, LANES, row_width), BF16),
            pltpu.VMEM((n_far, n_chunk, HALVES, LANES, narrow), BF16),
            pltpu.VMEM((n_far, n_chunk // 2, HALVES, LANES, narrow), BF16),
            pltpu.VMEM((n_col, n_chunk // 2, LANES, row_width), BF16),
            pltpu.VMEM((n_chip // 2, n_kb, LANES, row_width), BF16),
            dma((PIECES, n_row)),
            dma((PIECES, n_row)),
            dma((n_col, n_chunk)),
            dma((n_col, n_chunk)),
            dma((n_col, n_chunk)),
            dma((n_col, n_chunk)),
            dma((n_col, n_chunk // 2)),
            dma((n_far, n_chunk, HALVES)),
            dma((n_far, n_chunk // 2, HALVES)),
            dma((n_col, n_chunk, HALVES)),
            dma((n_col, n_chunk // 2, HALVES)),
            dma((n_col, n_chunk, HALVES)),
            dma((n_chip // 2, n_kb, HALVES)),
            dma((n_far, n_chunk, HALVES)),
            dma((n_far, n_chunk, HALVES)),
            dma((PIECES,)),
            dma((PIECES,)),
        ],
        compiler_params=pltpu.CompilerParams(
            collective_id=0, has_side_effects=True, vmem_limit_bytes=62 << 20
        ),
    )(meta, offsets, weight, integrals, coeffs)


def solution(mesh):
    in_specs = (P("row", None, "col"), P("row", "col"), P(), P(), P())
    out_specs = P("row", "col")
    return jax.shard_map(body, mesh=mesh, in_specs=in_specs, out_specs=out_specs, check_vma=False)
```

```python
import functools

import jax
import jax.numpy as jnp
from jax import lax
from jax.experimental import pallas as pl
from jax.experimental.pallas import tpu as pltpu
from jax.sharding import PartitionSpec as P

MESH = pl.DeviceIdType.MESH
F32 = jnp.float32
BF16 = jnp.bfloat16
LANES = 128
EARLY = 2
PIECES = 4
HALVES = 2
JOIN = 2
LAG = 4
PASS_LAG = 2


def remote(src, dst, send, recv, device):
    return pltpu.make_async_remote_copy(
        src_ref=src, dst_ref=dst, send_sem=send, recv_sem=recv, device_id=device, device_id_type=MESH
    )


def nearest(me, n, s):
    m = jnp.minimum(me, n - 1 - me)
    step = (s + 1) // 2
    near = jnp.where(s % 2 == 1, me - step, me + step)
    far = jnp.where(me <= n - 1 - me, s, n - 1 - s)
    return jnp.where(s <= 2 * m, near, far)


def kernel(n_row, n_col, cap, n_chunk, *refs):
    meta, offsets, mask, integrals, coeffs, out = refs[:6]
    asend, arecv = refs[6 : 6 + PIECES], refs[6 + PIECES : 6 + 2 * PIECES]
    (
        kept, kept_end, gathered, work, core_in, work_far, core_far, pair, sums,
        a_ss, a_rs, r_ss, l_ss, g_rs, c_ss, c_rs, d_ss, d_rs, p_ss, p_rs, t_ss, t_rs, f_ss, f_rs, k_ss, k_rs,
    ) = refs[6 + 2 * PIECES :]
    me = lax.axis_index("row")
    plane = lax.axis_index("col")
    core = me % 2
    chip = me // 2
    n_chip = n_row // 2
    partner = me + 1 - 2 * core
    buddy = chip + 1 - 2 * (chip % 2)
    per_dev, atom_w, row_width = integrals.shape
    half = atom_w // 2
    pairs = per_dev // 2
    packed = 3 * half
    slots = n_row * cap
    per_plane = n_row // n_col
    chips_plane = per_plane // 2
    n_kb = n_chunk // per_plane
    piece = row_width // PIECES
    half_width = row_width // HALVES
    per_half = PIECES // HALVES
    n_far = n_col - 2
    inner = n_col - 2
    has_left = plane > 0
    has_right = plane < n_col - 1
    is_end = (plane == 0) | (plane == n_col - 1)
    is_helper = (plane == 1) | (plane == n_col - 2)
    low_half = plane <= n_col - 1 - plane
    near_end = jnp.where(low_half, 0, n_col - 1)
    far_end = n_col - 1 - near_end
    helper_plane = jnp.where(low_half, 1, n_col - 2)

    barrier = pltpu.get_barrier_semaphore()
    for other in range(1, n_row):
        pl.semaphore_signal(barrier, inc=1, device_id=((me + other) % n_row, plane), device_id_type=MESH)

    @pl.when(has_left)
    def _():
        pl.semaphore_signal(barrier, inc=1, device_id=(me, plane - 1), device_id_type=MESH)

    @pl.when(has_right)
    def _():
        pl.semaphore_signal(barrier, inc=1, device_id=(me, plane + 1), device_id_type=MESH)

    def selection(p, weighted):
        s = lax.broadcasted_iota(jnp.int32, (packed, 2 * atom_w), 0)
        t = lax.broadcasted_iota(jnp.int32, (packed, 2 * atom_w), 1)
        first = me * per_dev + 2 * p
        extra = offsets[first + 1] - offsets[first] - half
        source = jnp.where(
            s < half, s, jnp.where(s < 2 * half, s + half, jnp.where(s - 2 * half < extra, s - half, s + half - extra))
        )
        hit = source == t
        if weighted:
            sig = jnp.where(t < atom_w, mask[plane, first], mask[plane, first + 1])
            hit = hit & (sig > 0)
        return jnp.where(hit, 1.0, 0.0).astype(BF16)

    def column(n):
        return ((n % per_plane) * n_kb + n // per_plane) * LANES

    def pack_coeffs(chunks):
        def pack(p, carry):
            at = pl.ds(pl.multiple_of(p * packed, 16), packed)
            rows = pl.ds(pl.multiple_of(p * 2 * atom_w, 2 * atom_w), 2 * atom_w)
            pick = selection(p, False)
            live = jnp.concatenate([coeffs[rows, column(n) : column(n) + LANES] for n in chunks], axis=1)
            live = jnp.dot(pick, live, preferred_element_type=F32).astype(BF16)
            for i, n in enumerate(chunks):
                gathered[plane, n, at, :] = live[:, i * LANES : (i + 1) * LANES]
            return carry

        lax.fori_loop(0, pairs, pack, 0, unroll=4)

    def to_right(z, n):
        return remote(gathered.at[z, n], gathered.at[z, n], r_ss.at[z], g_rs.at[z, n], (me, plane + 1))

    def to_left(z, n):
        return remote(gathered.at[z, n], gathered.at[z, n], l_ss.at[z], g_rs.at[z, n], (me, plane - 1))

    def goes_right(z):
        return (z <= plane) & has_right & ((plane != n_col - 2) | (z == plane))

    def goes_left(z):
        return (z >= plane) & has_left & ((plane != 1) | (z == plane))

    def forward(z, n):
        @pl.when(goes_right(z))
        def _():
            to_right(z, n).start()

        @pl.when(goes_left(z))
        def _():
            to_left(z, n).start()

    early = min(EARLY, n_chunk)
    pack_coeffs(range(early))
    pl.semaphore_wait(barrier, n_row - 1 + has_left.astype(jnp.int32) + has_right.astype(jnp.int32))
    for n in range(early):
        forward(plane, n)

    def a_copy(q, owner):
        return remote(asend[q].at[owner], arecv[q].at[me], a_ss.at[q, owner], a_rs.at[q, me], (owner, plane))

    for q in range(PIECES):
        lanes = slice(q * piece, (q + 1) * piece)

        def place(step, carry):
            owner = (me + step) % n_row

            @pl.when(step > 0)
            def _():
                for c in range(cap):
                    asend[q][owner, c] = integrals[meta[owner * cap + c], :, lanes]
                a_copy(q, owner).start()

            @pl.when(step == 0)
            def _():
                for c in range(cap):
                    arecv[q][me, c] = integrals[meta[me * cap + c], :, lanes]

            return carry

        lax.fori_loop(0, n_row, place, 0)

    if early < n_chunk:
        pack_coeffs(range(early, n_chunk))

        @pl.when(jnp.logical_not(is_end))
        def _():
            for n in range(early, n_chunk):
                forward(plane, n)

    def kept_copy(q):
        lanes, there = pl.ds(q * piece, piece), pl.ds(q % per_half * piece, piece)
        return remote(
            kept.at[:, lanes], kept_end.at[q // per_half, :, there], k_ss.at[q], k_rs.at[q], (me, helper_plane)
        )

    for q in range(PIECES):
        lanes = slice(q * piece, (q + 1) * piece)

        def wait_blocks(step, carry):
            source = (me + step) % n_row
            remote(
                asend[q].at[source], arecv[q].at[source], a_ss.at[q, source], a_rs.at[q, source], (source, plane)
            ).wait_recv()
            return carry

        lax.fori_loop(1, n_row, wait_blocks, 0)

        def pack_kept(p, carry):
            first, second = meta[slots + 2 * p], meta[slots + 2 * p + 1]
            rows = jnp.concatenate(
                [arecv[q][first // cap, first % cap], arecv[q][second // cap, second % cap]], axis=0
            )
            live = jnp.dot(selection(p, True), rows, preferred_element_type=F32).astype(BF16)
            kept[pl.ds(pl.multiple_of(p * packed, 16), packed), lanes] = live
            return carry

        lax.fori_loop(0, pairs, pack_kept, 0, unroll=4)

        @pl.when(is_end)
        def _():
            kept_copy(q).start()

    def kept_copy_in(h, i):
        q, there = h * per_half + i, pl.ds(i * piece, piece)
        return remote(
            kept.at[:, there], kept_end.at[h, :, there], k_ss.at[q], k_rs.at[q], (me, helper_plane)
        )

    @pl.when(is_end)
    def _():
        for n in range(early, n_chunk):
            forward(plane, n)

    def arrive(z, n):
        to_right(z, n).wait_recv()
        forward(z, n)

    @pl.when(jnp.logical_not(is_end))
    def _():
        for n in range(early):
            arrive(near_end, n)

    inside = inner * (n_chunk // 2)
    per_pass = (n_far - 1) * (n_chunk // 2)
    one = inside + per_pass
    two = one + early // 2
    three = two + (HALVES - 1) * per_pass
    group = 2 + HALVES
    steps = jnp.where(is_end, n_chunk, three + group * n_chunk)
    beside = jnp.where(low_half, 1, n_col - 2)

    def far_plane(f):
        return jnp.where(low_half, f + 2, n_col - 3 - f)

    def decode(s):
        first = s < inside
        last = s >= three
        near_wide = (s >= one) & (s < two)
        far_wide = jnp.logical_not(first | last | near_wide)
        v = jnp.where(s < one, s - inside, s - two + per_pass)
        u = s - three
        m, r = u // group + 1, u % group
        near = last & (r == 0)
        far_single = last & (r > 0) & (r <= HALVES)
        far = (far_wide | far_single) & jnp.logical_not(is_end)
        z = jnp.where(
            first, 1 + nearest(plane - 1, inner, s % inner), jnp.where(near_wide | near, near_end, far_end)
        )
        n = jnp.where(
            first,
            s // inner * 2,
            jnp.where(near_wide, (s - one) * 2, jnp.where(far_wide, v % (n_chunk // 2) * 2, jnp.where(near, m, m - 1))),
        )
        f = jnp.where(far_wide, v % per_pass // (n_chunk // 2), n_far - 1)
        h = jnp.where(far_wide, v // per_pass, r - 1)
        z = jnp.where(far, far_plane(f), z)
        late = last & (n < n_chunk) & (jnp.logical_not(near) | (n >= early))
        valid = first | near_wide | (far_wide & is_helper) | (late & (is_helper | jnp.logical_not(far_single)))
        comes = (first & (z != plane)) | (late & (r <= 1))
        z = jnp.where(is_end, jnp.where(s % 2 == 0, plane, beside), z)
        n = jnp.where(is_end, s // 2 * 2, n)
        comes = jnp.where(is_end, s % 2 == 1, comes)
        wide = jnp.logical_not(last) | is_end
        running = (s >= 0) & (s < steps)
        valid = (valid | is_end) & running
        n = jnp.clip(n, 0, n_chunk - 1)
        h = jnp.clip(h, 0, HALVES - 1)
        return valid & jnp.logical_not(far), valid & far, comes & running, wide, z, n, f, h

    def mine(wide, n):
        return wide | (n % 2 == core), jnp.where(wide, n + core, n)

    def other(wide, n):
        return wide | (n % 2 != core), jnp.where(wide, n + 1 - core, n)

    def core_copy(z, n):
        return remote(work.at[z, n], core_in.at[z, n // 2], c_ss, c_rs.at[z, n // 2], (partner, plane))

    def far_core_copy(f, n, h):
        return remote(
            work_far.at[f, n, h], core_far.at[f, n // 2, h], d_ss, d_rs.at[f, n // 2, h], (partner, plane)
        )

    def far_copy(f, z, n, h, to):
        lanes = pl.ds(pl.multiple_of(h * half_width, LANES), half_width)
        return remote(work_far.at[f, n, h], work.at[z, n, :, lanes], f_ss, f_rs.at[f, n, h], (me, to))

    def target(z, n):
        return z * chips_plane + (n % per_plane) // 2

    def half_lanes(h):
        return pl.ds(pl.multiple_of(h * half_width, LANES), half_width)

    def pair_copy(z, n, h):
        return remote(
            work.at[z, n, :, half_lanes(h)], pair.at[z, n // 2, :, half_lanes(h)], p_ss,
            p_rs.at[z, n // 2, h], (2 * buddy + core, plane),
        )

    def target_copy(z, n, h):
        return remote(
            work.at[z, n, :, half_lanes(h)], sums.at[chip // 2, n // per_plane, :, half_lanes(h)], t_ss,
            t_rs.at[chip // 2, n // per_plane, h], (2 * target(z, n) + core, plane),
        )

    def sends_pair(z, n):
        return target(z, n) % 2 != chip % 2

    def sends_sum(z, n):
        return (target(z, n) % 2 == chip % 2) & (target(z, n) != chip)

    def multiply(lhs, rhs):
        return lax.dot_general(lhs, rhs, (((0,), (0,)), ((), ())), preferred_element_type=F32).astype(BF16)

    def add(x, y):
        return (x.astype(F32) + y.astype(F32)).astype(BF16)

    def compute(s):
        own, far, comes, wide, z, n, f, h = decode(s)

        @pl.when(comes)
        def _():
            arrive(z, n)

            @pl.when(wide)
            def _():
                arrive(z, n + 1)

        def both():
            return jnp.concatenate([gathered[z, n], gathered[z, n + 1]], axis=1)

        @pl.when(own & wide)
        def _():
            part = multiply(both(), kept[...])
            work[z, n] = part[:LANES]
            work[z, n + 1] = part[LANES:]

        @pl.when(own & jnp.logical_not(wide))
        def _():
            work[z, n] = multiply(gathered[z, n], kept[...])

        @pl.when(far & wide)
        def _():
            @pl.when((f == 0) & (n == 0))
            def _():
                for i in range(per_half):
                    kept_copy_in(h, i).wait_recv()

            part = multiply(both(), kept_end[h])
            work_far[f, n, h] = part[:LANES]
            work_far[f, n + 1, h] = part[LANES:]

        @pl.when(far & jnp.logical_not(wide))
        def _():
            work_far[f, n, h] = multiply(gathered[z, n], kept_end[h])

        there, n_other = other(wide, n)

        @pl.when(own & there)
        def _():
            core_copy(z, n_other).start()

        @pl.when(far & there)
        def _():
            far_core_copy(f, n_other, h).start()

    def join_cores(s):
        own, far, comes, wide, z, n, f, h = decode(s)
        here, n = mine(wide, n)

        @pl.when(own & here)
        def _():
            core_copy(z, n).wait_recv()
            work[z, n] = add(work[z, n], core_in[z, n // 2])

            @pl.when(sends_pair(z, n))
            def _():
                for i in range(HALVES):
                    pair_copy(z, n, i).start()

        @pl.when(far & here)
        def _():
            far_core_copy(f, n, h).wait_recv()
            work_far[f, n, h] = add(work_far[f, n, h], core_far[f, n // 2, h])
            far_copy(f, z, n, h, near_end).start()

    def join_chips(s, carry):
        own, far, comes, wide, z, n, f, h = decode(s)
        here, n = mine(wide, n)

        @pl.when(own & here & sends_sum(z, n))
        def _():
            for i in range(HALVES):
                pair_copy(z, n, i).wait_recv()
                lanes = pl.ds(i * half_width, half_width)
                work[z, n, :, lanes] = add(work[z, n, :, lanes], pair[z, n // 2, :, lanes])
                target_copy(z, n, i).start()

        return carry

    def joined(s):
        return jnp.clip(jnp.minimum(2 * (s - three + 1), s - LAG), 0, steps)

    def step_body(s, carry):
        compute(s)
        join_cores(s - JOIN)
        lax.fori_loop(joined(s - 1), joined(s), join_chips, 0)
        return carry

    lax.fori_loop(0, steps + JOIN, step_body, 0)
    lax.fori_loop(joined(steps + JOIN - 1), steps, join_chips, 0)

    n_pass = n_far * n_chunk * HALVES

    def passed(e):
        v = e % ((n_far - 1) * n_chunk)
        w = e - (n_far - 1) * n_chunk * HALVES
        f = jnp.where(w < 0, v // n_chunk, n_far - 1)
        n = jnp.where(w < 0, v % n_chunk, w // HALVES)
        h = jnp.where(w < 0, e // ((n_far - 1) * n_chunk), w % HALVES)
        return f, far_plane(f), n, h

    @pl.when(is_end)
    def _():
        def pass_on(e, carry):
            @pl.when(e < n_pass)
            def _():
                f, z, n, h = passed(e)

                @pl.when(n % 2 == core)
                def _():
                    far_copy(f, z, n, h, plane).wait_recv()

                    @pl.when(sends_pair(z, n))
                    def _():
                        pair_copy(z, n, h).start()

            @pl.when(e >= PASS_LAG)
            def _():
                f, z, n, h = passed(e - PASS_LAG)

                @pl.when((n % 2 == core) & sends_sum(z, n))
                def _():
                    pair_copy(z, n, h).wait_recv()
                    lanes = half_lanes(h)
                    work[z, n, :, lanes] = add(work[z, n, :, lanes], pair[z, n // 2, :, lanes])
                    target_copy(z, n, h).start()

            return carry

        lax.fori_loop(0, n_pass + PASS_LAG, pass_on, 0)

    own_z, own_b = me // per_plane, me % per_plane
    for kb in range(n_kb):
        n = kb * per_plane + own_b
        for h in range(HALVES):
            pair_copy(own_z, n, h).wait_recv()
        total = work[own_z, n].astype(F32) + pair[own_z, n // 2].astype(F32)
        for step in range(1, n_chip // 2):
            source = (chip // 2 + step) % (n_chip // 2)
            for h in range(HALVES):
                remote(
                    work.at[own_z, n, :, half_lanes(h)], sums.at[source, kb, :, half_lanes(h)], t_ss,
                    t_rs.at[source, kb, h], (2 * (2 * source + chip % 2) + core, plane),
                ).wait_recv()
            total += sums[source, kb].astype(F32)
        out[kb * LANES : (kb + 1) * LANES, :] = total.astype(BF16)

    def drain_blocks(step, carry):
        for q in range(PIECES):
            a_copy(q, (me + step) % n_row).wait_send()
        return carry

    lax.fori_loop(1, n_row, drain_blocks, 0)

    def sent(ref, sem):
        remote(ref, ref, sem, sem, (partner, plane)).wait_send()

    sent(pair.at[: n_col // 2], p_ss)
    if n_chip > 2:
        sent(sums.at[: n_chip // 2 - 1], t_ss)

    @pl.when(is_end)
    def _():
        sent(core_in.at[:2], c_ss)
        for q in range(PIECES):
            kept_copy(q).wait_send()

    @pl.when(jnp.logical_not(is_end))
    def _():
        sent(core_in, c_ss)

    @pl.when(is_helper)
    def _():
        sent(core_far, d_ss)
        sent(core_far, f_ss)

    def drain_gathered(z, carry):
        @pl.when(goes_right(z))
        def _():
            sent(gathered.at[z], r_ss.at[z])

        @pl.when(goes_left(z))
        def _():
            sent(gathered.at[z], l_ss.at[z])

        return carry

    lax.fori_loop(0, n_col, drain_gathered, 0)


def body(integrals, coeffs, mask, offsets, atom_of_slot):
    n_row = lax.axis_size("row")
    n_col = lax.axis_size("col")
    me = lax.axis_index("row")
    per_dev, atom_w, row_width = integrals.shape
    rows, cols = coeffs.shape
    cap = max(2, -(-per_dev // n_row))
    slots = n_row * cap
    block = cols * n_col // n_row
    n_chunk = cols // LANES
    n_kb = block // LANES

    n_atom = atom_of_slot.shape[0]

    slot = jnp.arange(n_atom, dtype=jnp.int32)
    owner = atom_of_slot // per_dev
    holder = slot // per_dev
    flow = holder * n_row + owner
    rank = jnp.sum(((flow[None, :] == flow[:, None]) & (slot[None, :] < slot[:, None])).astype(jnp.int32), axis=1)
    goes = jnp.where(holder == me, owner * cap + rank, -1)
    comes = atom_of_slot - me * per_dev + slots
    entry = jnp.arange(slots + per_dev, dtype=jnp.int32)[:, None]
    meta = jnp.sum(
        jnp.where(
            entry < slots,
            jnp.where(goes[None, :] == entry, (slot - me * per_dev)[None, :], 0),
            jnp.where(comes[None, :] == entry, (holder * cap + rank)[None, :], 0),
        ),
        axis=1,
    )

    packed = rows * 3 // 4
    dma = pltpu.SemaphoreType.DMA
    n_chip = n_row // 2
    n_far = n_col - 2
    narrow = row_width // HALVES
    moved = [pltpu.VMEM((n_row, cap, atom_w, row_width // PIECES), BF16)] * (2 * PIECES)
    smem = pl.BlockSpec(memory_space=pltpu.SMEM)
    vmem = pl.BlockSpec(memory_space=pltpu.VMEM)
    return pl.pallas_call(
        functools.partial(kernel, n_row, n_col, cap, n_chunk),
        out_shape=jax.ShapeDtypeStruct((block, row_width), BF16),
        in_specs=[smem, smem, smem, vmem, vmem],
        out_specs=vmem,
        scratch_shapes=moved
        + [
            pltpu.VMEM((packed, row_width), BF16),
            pltpu.VMEM((HALVES, packed, narrow), BF16),
            pltpu.VMEM((n_col, n_chunk, packed, LANES), BF16),
            pltpu.VMEM((n_col, n_chunk, LANES, row_width), BF16),
            pltpu.VMEM((n_col, n_chunk // 2, LANES, row_width), BF16),
            pltpu.VMEM((n_far, n_chunk, HALVES, LANES, narrow), BF16),
            pltpu.VMEM((n_far, n_chunk // 2, HALVES, LANES, narrow), BF16),
            pltpu.VMEM((n_col, n_chunk // 2, LANES, row_width), BF16),
            pltpu.VMEM((n_chip // 2, n_kb, LANES, row_width), BF16),
            dma((PIECES, n_row)),
            dma((PIECES, n_row)),
            dma((n_col,)),
            dma((n_col,)),
            dma((n_col, n_chunk)),
            dma,
            dma((n_col, n_chunk // 2)),
            dma,
            dma((n_far, n_chunk // 2, HALVES)),
            dma,
            dma((n_col, n_chunk // 2, HALVES)),
            dma,
            dma((n_chip // 2, n_kb, HALVES)),
            dma,
            dma((n_far, n_chunk, HALVES)),
            dma((PIECES,)),
            dma((PIECES,)),
        ],
        compiler_params=pltpu.CompilerParams(
            collective_id=0, has_side_effects=True, vmem_limit_bytes=62 << 20
        ),
    )(meta, offsets, mask.T, integrals, coeffs)


def solution(mesh):
    in_specs = (P("row", None, "col"), P("row", "col"), P(), P(), P())
    out_specs = P("row", "col")
    return jax.shard_map(body, mesh=mesh, in_specs=in_specs, out_specs=out_specs, check_vma=False)
```

```python
import functools

import jax
import jax.numpy as jnp
from jax import lax
from jax.experimental import pallas as pl
from jax.experimental.pallas import tpu as pltpu
from jax.sharding import PartitionSpec as P

MESH = pl.DeviceIdType.MESH
F32 = jnp.float32
BF16 = jnp.bfloat16
LANES = 128
EARLY = 2
PIECES = 4
HALVES = 2
PARTS = 1
JOIN = 2
LAG = 4
PASS_LAG = 2


def remote(src, dst, send, recv, device):
    return pltpu.make_async_remote_copy(
        src_ref=src, dst_ref=dst, send_sem=send, recv_sem=recv, device_id=device, device_id_type=MESH
    )


def nearest(me, n, s):
    m = jnp.minimum(me, n - 1 - me)
    step = (s + 1) // 2
    near = jnp.where(s % 2 == 1, me - step, me + step)
    far = jnp.where(me <= n - 1 - me, s, n - 1 - s)
    return jnp.where(s <= 2 * m, near, far)


def kernel(n_row, n_col, cap, n_chunk, *refs):
    meta, offsets, mask, integrals, coeffs, out = refs[:6]
    asend, arecv = refs[6 : 6 + PIECES], refs[6 + PIECES : 6 + 2 * PIECES]
    (
        kept, kept_end, gathered, work, core_in, work_far, core_far, pair, sums,
        a_ss, a_rs, r_ss, l_ss, g_rs, c_ss, c_rs, d_ss, d_rs, p_ss, p_rs, t_ss, t_rs, f_ss, f_rs, k_ss, k_rs,
    ) = refs[6 + 2 * PIECES :]
    me = lax.axis_index("row")
    plane = lax.axis_index("col")
    core = me % 2
    chip = me // 2
    n_chip = n_row // 2
    partner = me + 1 - 2 * core
    buddy = chip + 1 - 2 * (chip % 2)
    per_dev, atom_w, row_width = integrals.shape
    half = atom_w // 2
    pairs = per_dev // 2
    packed = 3 * half
    slots = n_row * cap
    per_plane = n_row // n_col
    chips_plane = per_plane // 2
    n_kb = n_chunk // per_plane
    piece = row_width // PIECES
    half_width = row_width // HALVES
    per_half = PIECES // HALVES
    n_far = n_col - 2
    inner = n_col - 2
    has_left = plane > 0
    has_right = plane < n_col - 1
    is_end = (plane == 0) | (plane == n_col - 1)
    is_helper = (plane == 1) | (plane == n_col - 2)
    low_half = plane <= n_col - 1 - plane
    near_end = jnp.where(low_half, 0, n_col - 1)
    far_end = n_col - 1 - near_end
    helper_plane = jnp.where(low_half, 1, n_col - 2)

    barrier = pltpu.get_barrier_semaphore()
    for other in range(1, n_row):
        pl.semaphore_signal(barrier, inc=1, device_id=((me + other) % n_row, plane), device_id_type=MESH)

    @pl.when(has_left)
    def _():
        pl.semaphore_signal(barrier, inc=1, device_id=(me, plane - 1), device_id_type=MESH)

    @pl.when(has_right)
    def _():
        pl.semaphore_signal(barrier, inc=1, device_id=(me, plane + 1), device_id_type=MESH)

    def selection(p, weighted):
        s = lax.broadcasted_iota(jnp.int32, (packed, 2 * atom_w), 0)
        t = lax.broadcasted_iota(jnp.int32, (packed, 2 * atom_w), 1)
        first = me * per_dev + 2 * p
        extra = offsets[first + 1] - offsets[first] - half
        source = jnp.where(
            s < half, s, jnp.where(s < 2 * half, s + half, jnp.where(s - 2 * half < extra, s - half, s + half - extra))
        )
        hit = source == t
        if weighted:
            sig = jnp.where(t < atom_w, mask[plane, first], mask[plane, first + 1])
            hit = hit & (sig > 0)
        return jnp.where(hit, 1.0, 0.0).astype(BF16)

    def column(n):
        return ((n % per_plane) * n_kb + n // per_plane) * LANES

    def pack_coeffs(chunks):
        def pack(p, carry):
            at = pl.ds(pl.multiple_of(p * packed, 16), packed)
            rows = pl.ds(pl.multiple_of(p * 2 * atom_w, 2 * atom_w), 2 * atom_w)
            pick = selection(p, False)
            live = jnp.concatenate([coeffs[rows, column(n) : column(n) + LANES] for n in chunks], axis=1)
            live = jnp.dot(pick, live, preferred_element_type=F32).astype(BF16)
            for i, n in enumerate(chunks):
                gathered[plane, n, at, :] = live[:, i * LANES : (i + 1) * LANES]
            return carry

        lax.fori_loop(0, pairs, pack, 0, unroll=4)

    def part_of(z, n, i):
        return gathered.at[z, n, pl.ds(i * (pairs * packed // PARTS), pairs * packed // PARTS)]

    def to_right(z, n, i):
        return remote(part_of(z, n, i), part_of(z, n, i), r_ss.at[z], g_rs.at[z, n, i], (me, plane + 1))

    def to_left(z, n, i):
        return remote(part_of(z, n, i), part_of(z, n, i), l_ss.at[z], g_rs.at[z, n, i], (me, plane - 1))

    def goes_right(z):
        return (z <= plane) & has_right & ((plane != n_col - 2) | (z == plane))

    def goes_left(z):
        return (z >= plane) & has_left & ((plane != 1) | (z == plane))

    def forward(z, n, parts=range(PARTS)):
        @pl.when(goes_right(z))
        def _():
            for i in parts:
                to_right(z, n, i).start()

        @pl.when(goes_left(z))
        def _():
            for i in parts:
                to_left(z, n, i).start()

    early = min(EARLY, n_chunk)
    pack_coeffs(range(early))
    pl.semaphore_wait(barrier, n_row - 1 + has_left.astype(jnp.int32) + has_right.astype(jnp.int32))
    for n in range(early):
        forward(plane, n)

    def a_copy(q, owner):
        return remote(asend[q].at[owner], arecv[q].at[me], a_ss.at[q, owner], a_rs.at[q, me], (owner, plane))

    for q in range(PIECES):
        lanes = slice(q * piece, (q + 1) * piece)

        def place(step, carry):
            owner = (me + step) % n_row

            @pl.when(step > 0)
            def _():
                for c in range(cap):
                    asend[q][owner, c] = integrals[meta[owner * cap + c], :, lanes]
                a_copy(q, owner).start()

            @pl.when(step == 0)
            def _():
                for c in range(cap):
                    arecv[q][me, c] = integrals[meta[me * cap + c], :, lanes]

            return carry

        lax.fori_loop(0, n_row, place, 0)

    if early < n_chunk:
        pack_coeffs(range(early, n_chunk))

        @pl.when(jnp.logical_not(is_end))
        def _():
            for n in range(early, n_chunk):
                forward(plane, n)

    def kept_copy(q):
        lanes, there = pl.ds(q * piece, piece), pl.ds(q % per_half * piece, piece)
        return remote(
            kept.at[:, lanes], kept_end.at[q // per_half, :, there], k_ss.at[q], k_rs.at[q], (me, helper_plane)
        )

    for q in range(PIECES):
        lanes = slice(q * piece, (q + 1) * piece)

        def wait_blocks(step, carry):
            source = (me + step) % n_row
            remote(
                asend[q].at[source], arecv[q].at[source], a_ss.at[q, source], a_rs.at[q, source], (source, plane)
            ).wait_recv()
            return carry

        lax.fori_loop(1, n_row, wait_blocks, 0)

        def pack_kept(p, carry):
            first, second = meta[slots + 2 * p], meta[slots + 2 * p + 1]
            rows = jnp.concatenate(
                [arecv[q][first // cap, first % cap], arecv[q][second // cap, second % cap]], axis=0
            )
            live = jnp.dot(selection(p, True), rows, preferred_element_type=F32).astype(BF16)
            kept[pl.ds(pl.multiple_of(p * packed, 16), packed), lanes] = live
            return carry

        lax.fori_loop(0, pairs, pack_kept, 0, unroll=4)

        @pl.when(is_end)
        def _():
            kept_copy(q).start()

    def kept_copy_in(h, i):
        q, there = h * per_half + i, pl.ds(i * piece, piece)
        return remote(
            kept.at[:, there], kept_end.at[h, :, there], k_ss.at[q], k_rs.at[q], (me, helper_plane)
        )

    @pl.when(is_end)
    def _():
        for n in range(early, n_chunk):
            forward(plane, n)

    def arrive(z, n):
        for i in range(PARTS):
            to_right(z, n, i).wait_recv()
            forward(z, n, [i])

    @pl.when(jnp.logical_not(is_end))
    def _():
        for n in range(early):
            arrive(near_end, n)

    inside = inner * (n_chunk // 2)
    per_pass = (n_far - 1) * (n_chunk // 2)
    one = inside + per_pass
    two = one + early // 2
    three = two + (HALVES - 1) * per_pass
    group = 2 + HALVES
    steps = jnp.where(is_end, n_chunk, three + group * n_chunk)
    beside = jnp.where(low_half, 1, n_col - 2)

    def far_plane(f):
        return jnp.where(low_half, f + 2, n_col - 3 - f)

    def reordered(s):
        if n_far != 2:
            return s
        own, far = inside - inner, per_pass - 1
        later = jnp.where(s < own + far + inner, s - far, s)
        return jnp.where(s < own, s, jnp.where(s < own + far, s + inner, later))

    def decode(at):
        running = (at >= 0) & (at < steps)
        s = jnp.where(is_end, at, reordered(at))
        first = s < inside
        last = s >= three
        near_wide = (s >= one) & (s < two)
        far_wide = jnp.logical_not(first | last | near_wide)
        v = jnp.where(s < one, s - inside, s - two + per_pass)
        u = s - three
        m, r = u // group, u % group
        near = last & (r == 0)
        far_single = last & (r > 0) & (r <= HALVES)
        far = (far_wide | far_single) & jnp.logical_not(is_end)
        z = jnp.where(
            first, 1 + nearest(plane - 1, inner, s % inner), jnp.where(near_wide | near, near_end, far_end)
        )
        n = jnp.where(
            first,
            s // inner * 2,
            jnp.where(near_wide, (s - one) * 2, jnp.where(far_wide, v % (n_chunk // 2) * 2, jnp.where(near, m + early, m))),
        )
        f = jnp.where(far_wide, v % per_pass // (n_chunk // 2), n_far - 1)
        h = jnp.where(far_wide, v // per_pass, r - 1)
        z = jnp.where(far, far_plane(f), z)
        late = last & (n < n_chunk)
        valid = first | near_wide | (far_wide & is_helper) | (late & (is_helper | jnp.logical_not(far_single)))
        comes = (first & (z != plane)) | (late & (r <= 1))
        z = jnp.where(is_end, jnp.where(s % 2 == 0, plane, beside), z)
        n = jnp.where(is_end, s // 2 * 2, n)
        comes = jnp.where(is_end, s % 2 == 1, comes)
        wide = jnp.logical_not(last) | is_end
        valid = (valid | is_end) & running
        n = jnp.clip(n, 0, n_chunk - 1)
        h = jnp.clip(h, 0, HALVES - 1)
        return valid & jnp.logical_not(far), valid & far, comes & running, wide, z, n, f, h

    def mine(wide, n):
        return wide | (n % 2 == core), jnp.where(wide, n + core, n)

    def other(wide, n):
        return wide | (n % 2 != core), jnp.where(wide, n + 1 - core, n)

    def core_copy(z, n):
        return remote(work.at[z, n], core_in.at[z, n // 2], c_ss, c_rs.at[z, n // 2], (partner, plane))

    def far_core_copy(f, n, h):
        return remote(
            work_far.at[f, n, h], core_far.at[f, n // 2, h], d_ss, d_rs.at[f, n // 2, h], (partner, plane)
        )

    def far_copy(f, z, n, h, to):
        lanes = pl.ds(pl.multiple_of(h * half_width, LANES), half_width)
        return remote(work_far.at[f, n, h], work.at[z, n, :, lanes], f_ss, f_rs.at[f, n, h], (me, to))

    def target(z, n):
        return z * chips_plane + (n % per_plane) // 2

    def half_lanes(h):
        return pl.ds(pl.multiple_of(h * half_width, LANES), half_width)

    def pair_copy(z, n, h):
        return remote(
            work.at[z, n, :, half_lanes(h)], pair.at[z, n // 2, :, half_lanes(h)], p_ss,
            p_rs.at[z, n // 2, h], (2 * buddy + core, plane),
        )

    def target_copy(z, n, h):
        return remote(
            work.at[z, n, :, half_lanes(h)], sums.at[chip // 2, n // per_plane, :, half_lanes(h)], t_ss,
            t_rs.at[chip // 2, n // per_plane, h], (2 * target(z, n) + core, plane),
        )

    def sends_pair(z, n):
        return target(z, n) % 2 != chip % 2

    def sends_sum(z, n):
        return (target(z, n) % 2 == chip % 2) & (target(z, n) != chip)

    def multiply(lhs, rhs):
        return lax.dot_general(lhs, rhs, (((0,), (0,)), ((), ())), preferred_element_type=F32).astype(BF16)

    def add(x, y):
        return (x.astype(F32) + y.astype(F32)).astype(BF16)

    def compute(s):
        own, far, comes, wide, z, n, f, h = decode(s)

        @pl.when(comes)
        def _():
            arrive(z, n)

            @pl.when(wide)
            def _():
                arrive(z, n + 1)

        def both():
            return jnp.concatenate([gathered[z, n], gathered[z, n + 1]], axis=1)

        @pl.when(own & wide)
        def _():
            part = multiply(both(), kept[...])
            work[z, n] = part[:LANES]
            work[z, n + 1] = part[LANES:]

        @pl.when(own & jnp.logical_not(wide))
        def _():
            work[z, n] = multiply(gathered[z, n], kept[...])

        @pl.when(far & wide)
        def _():
            @pl.when((f == 0) & (n == 0))
            def _():
                for i in range(per_half):
                    kept_copy_in(h, i).wait_recv()

            part = multiply(both(), kept_end[h])
            work_far[f, n, h] = part[:LANES]
            work_far[f, n + 1, h] = part[LANES:]

        @pl.when(far & jnp.logical_not(wide))
        def _():
            work_far[f, n, h] = multiply(gathered[z, n], kept_end[h])

        there, n_other = other(wide, n)

        @pl.when(own & there)
        def _():
            core_copy(z, n_other).start()

        @pl.when(far & there)
        def _():
            far_core_copy(f, n_other, h).start()

    def join_cores(s):
        own, far, comes, wide, z, n, f, h = decode(s)
        here, n = mine(wide, n)

        @pl.when(own & here)
        def _():
            core_copy(z, n).wait_recv()
            work[z, n] = add(work[z, n], core_in[z, n // 2])

            @pl.when(sends_pair(z, n))
            def _():
                for i in range(HALVES):
                    pair_copy(z, n, i).start()

        @pl.when(far & here)
        def _():
            far_core_copy(f, n, h).wait_recv()
            work_far[f, n, h] = add(work_far[f, n, h], core_far[f, n // 2, h])
            far_copy(f, z, n, h, near_end).start()

    def join_chips(s, carry):
        own, far, comes, wide, z, n, f, h = decode(s)
        here, n = mine(wide, n)

        @pl.when(own & here & sends_sum(z, n))
        def _():
            for i in range(HALVES):
                pair_copy(z, n, i).wait_recv()
                lanes = pl.ds(i * half_width, half_width)
                work[z, n, :, lanes] = add(work[z, n, :, lanes], pair[z, n // 2, :, lanes])
                target_copy(z, n, i).start()

        return carry

    def joined(s):
        return jnp.clip(jnp.minimum(2 * (s - three + 1), s - LAG), 0, steps)

    def step_body(s, carry):
        compute(s)
        join_cores(s - JOIN)
        lax.fori_loop(joined(s - 1), joined(s), join_chips, 0)
        return carry

    lax.fori_loop(0, steps + JOIN, step_body, 0)
    lax.fori_loop(joined(steps + JOIN - 1), steps, join_chips, 0)

    n_pass = n_far * n_chunk * HALVES

    def passed(e):
        v = e % ((n_far - 1) * n_chunk)
        w = e - (n_far - 1) * n_chunk * HALVES
        f = jnp.where(w < 0, v // n_chunk, n_far - 1)
        n = jnp.where(w < 0, v % n_chunk, w // HALVES)
        h = jnp.where(w < 0, e // ((n_far - 1) * n_chunk), w % HALVES)
        return f, far_plane(f), n, h

    @pl.when(is_end)
    def _():
        def pass_on(e, carry):
            @pl.when(e < n_pass)
            def _():
                f, z, n, h = passed(e)

                @pl.when(n % 2 == core)
                def _():
                    far_copy(f, z, n, h, plane).wait_recv()

                    @pl.when(sends_pair(z, n))
                    def _():
                        pair_copy(z, n, h).start()

            @pl.when(e >= PASS_LAG)
            def _():
                f, z, n, h = passed(e - PASS_LAG)

                @pl.when((n % 2 == core) & sends_sum(z, n))
                def _():
                    pair_copy(z, n, h).wait_recv()
                    lanes = half_lanes(h)
                    work[z, n, :, lanes] = add(work[z, n, :, lanes], pair[z, n // 2, :, lanes])
                    target_copy(z, n, h).start()

            return carry

        lax.fori_loop(0, n_pass + PASS_LAG, pass_on, 0)

    own_z, own_b = me // per_plane, me % per_plane
    for kb in range(n_kb):
        n = kb * per_plane + own_b
        for h in range(HALVES):
            pair_copy(own_z, n, h).wait_recv()
        total = work[own_z, n].astype(F32) + pair[own_z, n // 2].astype(F32)
        for step in range(1, n_chip // 2):
            source = (chip // 2 + step) % (n_chip // 2)
            for h in range(HALVES):
                remote(
                    work.at[own_z, n, :, half_lanes(h)], sums.at[source, kb, :, half_lanes(h)], t_ss,
                    t_rs.at[source, kb, h], (2 * (2 * source + chip % 2) + core, plane),
                ).wait_recv()
            total += sums[source, kb].astype(F32)
        out[kb * LANES : (kb + 1) * LANES, :] = total.astype(BF16)

    def drain_blocks(step, carry):
        for q in range(PIECES):
            a_copy(q, (me + step) % n_row).wait_send()
        return carry

    lax.fori_loop(1, n_row, drain_blocks, 0)

    def sent(ref, sem):
        remote(ref, ref, sem, sem, (partner, plane)).wait_send()

    sent(pair.at[: n_col // 2], p_ss)
    if n_chip > 2:
        sent(sums.at[: n_chip // 2 - 1], t_ss)

    @pl.when(is_end)
    def _():
        sent(core_in.at[:2], c_ss)
        for q in range(PIECES):
            kept_copy(q).wait_send()

    @pl.when(jnp.logical_not(is_end))
    def _():
        sent(core_in, c_ss)

    @pl.when(is_helper)
    def _():
        sent(core_far, d_ss)
        sent(core_far, f_ss)

    def drain_gathered(z, carry):
        @pl.when(goes_right(z))
        def _():
            sent(gathered.at[z], r_ss.at[z])

        @pl.when(goes_left(z))
        def _():
            sent(gathered.at[z], l_ss.at[z])

        return carry

    lax.fori_loop(0, n_col, drain_gathered, 0)


def body(integrals, coeffs, mask, offsets, atom_of_slot):
    n_row = lax.axis_size("row")
    n_col = lax.axis_size("col")
    me = lax.axis_index("row")
    per_dev, atom_w, row_width = integrals.shape
    rows, cols = coeffs.shape
    cap = max(2, -(-per_dev // n_row))
    slots = n_row * cap
    block = cols * n_col // n_row
    n_chunk = cols // LANES
    n_kb = block // LANES

    n_atom = atom_of_slot.shape[0]

    slot = jnp.arange(n_atom, dtype=jnp.int32)
    local = lax.optimization_barrier(atom_of_slot - me * per_dev)
    owner = (local + me * per_dev) // per_dev
    holder = slot // per_dev
    flow = holder * n_row + owner
    rank = jnp.sum(((flow[None, :] == flow[:, None]) & (slot[None, :] < slot[:, None])).astype(jnp.int32), axis=1)
    goes = jnp.where(holder == me, owner * cap + rank, -1)
    comes = local + slots
    entry = jnp.arange(slots + per_dev, dtype=jnp.int32)[:, None]
    meta = jnp.sum(
        jnp.where(
            entry < slots,
            jnp.where(goes[None, :] == entry, (slot - me * per_dev)[None, :], 0),
            jnp.where(comes[None, :] == entry, (holder * cap + rank)[None, :], 0),
        ),
        axis=1,
    )

    packed = rows * 3 // 4
    dma = pltpu.SemaphoreType.DMA
    n_chip = n_row // 2
    n_far = n_col - 2
    narrow = row_width // HALVES
    moved = [pltpu.VMEM((n_row, cap, atom_w, row_width // PIECES), BF16)] * (2 * PIECES)
    smem = pl.BlockSpec(memory_space=pltpu.SMEM)
    vmem = pl.BlockSpec(memory_space=pltpu.VMEM)
    return pl.pallas_call(
        functools.partial(kernel, n_row, n_col, cap, n_chunk),
        out_shape=jax.ShapeDtypeStruct((block, row_width), BF16),
        in_specs=[smem, smem, smem, vmem, vmem],
        out_specs=vmem,
        scratch_shapes=moved
        + [
            pltpu.VMEM((packed, row_width), BF16),
            pltpu.VMEM((HALVES, packed, narrow), BF16),
            pltpu.VMEM((n_col, n_chunk, packed, LANES), BF16),
            pltpu.VMEM((n_col, n_chunk, LANES, row_width), BF16),
            pltpu.VMEM((n_col, n_chunk // 2, LANES, row_width), BF16),
            pltpu.VMEM((n_far, n_chunk, HALVES, LANES, narrow), BF16),
            pltpu.VMEM((n_far, n_chunk // 2, HALVES, LANES, narrow), BF16),
            pltpu.VMEM((n_col, n_chunk // 2, LANES, row_width), BF16),
            pltpu.VMEM((n_chip // 2, n_kb, LANES, row_width), BF16),
            dma((PIECES, n_row)),
            dma((PIECES, n_row)),
            dma((n_col,)),
            dma((n_col,)),
            dma((n_col, n_chunk, PARTS)),
            dma,
            dma((n_col, n_chunk // 2)),
            dma,
            dma((n_far, n_chunk // 2, HALVES)),
            dma,
            dma((n_col, n_chunk // 2, HALVES)),
            dma,
            dma((n_chip // 2, n_kb, HALVES)),
            dma,
            dma((n_far, n_chunk, HALVES)),
            dma((PIECES,)),
            dma((PIECES,)),
        ],
        compiler_params=pltpu.CompilerParams(
            collective_id=0, has_side_effects=True, vmem_limit_bytes=62 << 20
        ),
    )(meta, offsets, mask.T, integrals, coeffs)


def solution(mesh):
    in_specs = (P("row", None, "col"), P("row", "col"), P(), P(), P())
    out_specs = P("row", "col")
    return jax.shard_map(body, mesh=mesh, in_specs=in_specs, out_specs=out_specs, check_vma=False)
```

```python
import functools

import jax
import jax.numpy as jnp
from jax import lax
from jax.experimental import pallas as pl
from jax.experimental.pallas import tpu as pltpu
from jax.sharding import PartitionSpec as P

MESH = pl.DeviceIdType.MESH
F32 = jnp.float32
BF16 = jnp.bfloat16
LANES = 128
EARLY = 2
PIECES = 4
HALVES = 2
PARTS = 1
JOIN = 1
LAG = 3
PASS_LAG = 2


def remote(src, dst, send, recv, device):
    return pltpu.make_async_remote_copy(
        src_ref=src, dst_ref=dst, send_sem=send, recv_sem=recv, device_id=device, device_id_type=MESH
    )


def nearest(me, n, s):
    m = jnp.minimum(me, n - 1 - me)
    step = (s + 1) // 2
    near = jnp.where(s % 2 == 1, me - step, me + step)
    far = jnp.where(me <= n - 1 - me, s, n - 1 - s)
    return jnp.where(s <= 2 * m, near, far)


def kernel(n_row, n_col, cap, n_chunk, *refs):
    meta, offsets, mask, integrals, coeffs, out = refs[:6]
    asend, arecv = refs[6 : 6 + PIECES], refs[6 + PIECES : 6 + 2 * PIECES]
    (
        kept, kept_end, gathered, work, core_in, work_far, core_far, pair, sums,
        a_ss, a_rs, r_ss, l_ss, g_rs, c_ss, c_rs, d_ss, d_rs, p_ss, p_rs, t_ss, t_rs, f_ss, f_rs, k_ss, k_rs,
    ) = refs[6 + 2 * PIECES :]
    me = lax.axis_index("row")
    plane = lax.axis_index("col")
    core = me % 2
    chip = me // 2
    n_chip = n_row // 2
    partner = me + 1 - 2 * core
    buddy = chip + 1 - 2 * (chip % 2)
    per_dev, atom_w, row_width = integrals.shape
    half = atom_w // 2
    pairs = per_dev // 2
    packed = 3 * half
    slots = n_row * cap
    per_plane = n_row // n_col
    chips_plane = per_plane // 2
    n_kb = n_chunk // per_plane
    piece = row_width // PIECES
    half_width = row_width // HALVES
    per_half = PIECES // HALVES
    n_far = n_col - 2
    inner = n_col - 2
    has_left = plane > 0
    has_right = plane < n_col - 1
    is_end = (plane == 0) | (plane == n_col - 1)
    is_helper = (plane == 1) | (plane == n_col - 2)
    low_half = plane <= n_col - 1 - plane
    near_end = jnp.where(low_half, 0, n_col - 1)
    far_end = n_col - 1 - near_end
    helper_plane = jnp.where(low_half, 1, n_col - 2)

    barrier = pltpu.get_barrier_semaphore()
    for other in range(1, n_row):
        pl.semaphore_signal(barrier, inc=1, device_id=((me + other) % n_row, plane), device_id_type=MESH)

    @pl.when(has_left)
    def _():
        pl.semaphore_signal(barrier, inc=1, device_id=(me, plane - 1), device_id_type=MESH)

    @pl.when(has_right)
    def _():
        pl.semaphore_signal(barrier, inc=1, device_id=(me, plane + 1), device_id_type=MESH)

    def selection(p, weighted):
        s = lax.broadcasted_iota(jnp.int32, (packed, 2 * atom_w), 0)
        t = lax.broadcasted_iota(jnp.int32, (packed, 2 * atom_w), 1)
        first = me * per_dev + 2 * p
        extra = offsets[first + 1] - offsets[first] - half
        source = jnp.where(
            s < half, s, jnp.where(s < 2 * half, s + half, jnp.where(s - 2 * half < extra, s - half, s + half - extra))
        )
        hit = source == t
        if weighted:
            sig = jnp.where(t < atom_w, mask[plane, first], mask[plane, first + 1])
            hit = hit & (sig > 0)
        return jnp.where(hit, 1.0, 0.0).astype(BF16)

    def column(n):
        return ((n % per_plane) * n_kb + n // per_plane) * LANES

    def pack_coeffs(chunks):
        def pack(p, carry):
            at = pl.ds(pl.multiple_of(p * packed, 16), packed)
            rows = pl.ds(pl.multiple_of(p * 2 * atom_w, 2 * atom_w), 2 * atom_w)
            pick = selection(p, False)
            live = jnp.concatenate([coeffs[rows, column(n) : column(n) + LANES] for n in chunks], axis=1)
            live = jnp.dot(pick, live, preferred_element_type=F32).astype(BF16)
            for i, n in enumerate(chunks):
                gathered[plane, n, at, :] = live[:, i * LANES : (i + 1) * LANES]
            return carry

        lax.fori_loop(0, pairs, pack, 0, unroll=4)

    def part_of(z, n, i):
        return gathered.at[z, n, pl.ds(i * (pairs * packed // PARTS), pairs * packed // PARTS)]

    def to_right(z, n, i):
        return remote(part_of(z, n, i), part_of(z, n, i), r_ss.at[z], g_rs.at[z, n, i], (me, plane + 1))

    def to_left(z, n, i):
        return remote(part_of(z, n, i), part_of(z, n, i), l_ss.at[z], g_rs.at[z, n, i], (me, plane - 1))

    def goes_right(z):
        return (z <= plane) & has_right & ((plane != n_col - 2) | (z == plane))

    def goes_left(z):
        return (z >= plane) & has_left & ((plane != 1) | (z == plane))

    def forward(z, n, parts=range(PARTS)):
        @pl.when(goes_right(z))
        def _():
            for i in parts:
                to_right(z, n, i).start()

        @pl.when(goes_left(z))
        def _():
            for i in parts:
                to_left(z, n, i).start()

    early = min(EARLY, n_chunk)
    pack_coeffs(range(early))
    pl.semaphore_wait(barrier, n_row - 1 + has_left.astype(jnp.int32) + has_right.astype(jnp.int32))
    for n in range(early):
        forward(plane, n)

    def a_copy(q, owner):
        return remote(asend[q].at[owner], arecv[q].at[me], a_ss.at[q, owner], a_rs.at[q, me], (owner, plane))

    for q in range(PIECES):
        lanes = slice(q * piece, (q + 1) * piece)

        def place(step, carry):
            owner = (me + step) % n_row

            @pl.when(step > 0)
            def _():
                for c in range(cap):
                    asend[q][owner, c] = integrals[meta[owner * cap + c], :, lanes]
                a_copy(q, owner).start()

            @pl.when(step == 0)
            def _():
                for c in range(cap):
                    arecv[q][me, c] = integrals[meta[me * cap + c], :, lanes]

            return carry

        lax.fori_loop(0, n_row, place, 0)

    if early < n_chunk:
        pack_coeffs(range(early, n_chunk))

        @pl.when(jnp.logical_not(is_end))
        def _():
            for n in range(early, n_chunk):
                forward(plane, n)

    def kept_copy(q):
        lanes, there = pl.ds(q * piece, piece), pl.ds(q % per_half * piece, piece)
        return remote(
            kept.at[:, lanes], kept_end.at[q // per_half, :, there], k_ss.at[q], k_rs.at[q], (me, helper_plane)
        )

    for q in range(PIECES):
        lanes = slice(q * piece, (q + 1) * piece)

        def wait_blocks(step, carry):
            source = (me + step) % n_row
            remote(
                asend[q].at[source], arecv[q].at[source], a_ss.at[q, source], a_rs.at[q, source], (source, plane)
            ).wait_recv()
            return carry

        lax.fori_loop(1, n_row, wait_blocks, 0)

        def pack_kept(p, carry):
            first, second = meta[slots + 2 * p], meta[slots + 2 * p + 1]
            rows = jnp.concatenate(
                [arecv[q][first // cap, first % cap], arecv[q][second // cap, second % cap]], axis=0
            )
            live = jnp.dot(selection(p, True), rows, preferred_element_type=F32).astype(BF16)
            kept[pl.ds(pl.multiple_of(p * packed, 16), packed), lanes] = live
            return carry

        lax.fori_loop(0, pairs, pack_kept, 0, unroll=4)

        @pl.when(is_end)
        def _():
            kept_copy(q).start()

    def kept_copy_in(h, i):
        q, there = h * per_half + i, pl.ds(i * piece, piece)
        return remote(
            kept.at[:, there], kept_end.at[h, :, there], k_ss.at[q], k_rs.at[q], (me, helper_plane)
        )

    @pl.when(is_end)
    def _():
        for n in range(early, n_chunk):
            forward(plane, n)

    def arrive(z, n):
        for i in range(PARTS):
            to_right(z, n, i).wait_recv()
            forward(z, n, [i])

    @pl.when(jnp.logical_not(is_end))
    def _():
        for n in range(early):
            arrive(near_end, n)

    inside = inner * (n_chunk // 2)
    per_pass = (n_far - 1) * (n_chunk // 2)
    one = inside + per_pass
    two = one + early // 2
    three = two + (HALVES - 1) * per_pass
    group = 3
    steps = jnp.where(is_end, n_chunk, three + group * n_chunk)
    beside = jnp.where(low_half, 1, n_col - 2)

    def far_plane(f):
        return jnp.where(low_half, f + 2, n_col - 3 - f)

    def reordered(s):
        if n_far != 2:
            return s
        own, far = inside - inner, per_pass - 1
        later = jnp.where(s < own + far + inner, s - far, s)
        return jnp.where(s < own, s, jnp.where(s < own + far, s + inner, later))

    def decode(at):
        running = (at >= 0) & (at < steps)
        s = jnp.where(is_end, at, reordered(at))
        first = s < inside
        last = s >= three
        near_wide = (s >= one) & (s < two)
        far_wide = jnp.logical_not(first | last | near_wide)
        v = jnp.where(s < one, s - inside, s - two + per_pass)
        u = s - three
        m, r = u // group, u % group
        near = last & (r == 0)
        far_single = last & (r == 1)
        far = (far_wide | far_single) & jnp.logical_not(is_end)
        z = jnp.where(
            first, 1 + nearest(plane - 1, inner, s % inner), jnp.where(near_wide | near, near_end, far_end)
        )
        n = jnp.where(
            first,
            s // inner * 2,
            jnp.where(near_wide, (s - one) * 2, jnp.where(far_wide, v % (n_chunk // 2) * 2, jnp.where(near, m + early, m))),
        )
        f = jnp.where(far_wide, v % per_pass // (n_chunk // 2), n_far - 1)
        h = jnp.where(far_wide, v // per_pass, r - 1)
        z = jnp.where(far, far_plane(f), z)
        late = last & (n < n_chunk)
        valid = first | near_wide | (far_wide & is_helper) | (late & (is_helper | jnp.logical_not(far_single)))
        comes = (first & (z != plane)) | (late & (r <= 1))
        z = jnp.where(is_end, jnp.where(s % 2 == 0, plane, beside), z)
        n = jnp.where(is_end, s // 2 * 2, n)
        comes = jnp.where(is_end, s % 2 == 1, comes)
        wide = jnp.logical_not(last) | is_end
        valid = (valid | is_end) & running
        n = jnp.clip(n, 0, n_chunk - 1)
        h = jnp.clip(h, 0, HALVES - 1)
        return valid & jnp.logical_not(far), valid & far, comes & running, wide, z, n, f, h

    def mine(wide, n):
        return wide | (n % 2 == core), jnp.where(wide, n + core, n)

    def other(wide, n):
        return wide | (n % 2 != core), jnp.where(wide, n + 1 - core, n)

    def core_copy(z, n):
        return remote(work.at[z, n], core_in.at[z, n // 2], c_ss, c_rs.at[z, n // 2], (partner, plane))

    def far_core_copy(f, n, h):
        return remote(
            work_far.at[f, n, h], core_far.at[f, n // 2, h], d_ss, d_rs.at[f, n // 2, h], (partner, plane)
        )

    def far_copy(f, z, n, h, to):
        lanes = pl.ds(pl.multiple_of(h * half_width, LANES), half_width)
        return remote(work_far.at[f, n, h], work.at[z, n, :, lanes], f_ss, f_rs.at[f, n, h], (me, to))

    def target(z, n):
        return z * chips_plane + (n % per_plane) // 2

    def half_lanes(h):
        return pl.ds(pl.multiple_of(h * half_width, LANES), half_width)

    def pair_copy(z, n, h):
        return remote(
            work.at[z, n, :, half_lanes(h)], pair.at[z, n // 2, :, half_lanes(h)], p_ss,
            p_rs.at[z, n // 2, h], (2 * buddy + core, plane),
        )

    def target_copy(z, n, h):
        return remote(
            work.at[z, n, :, half_lanes(h)], sums.at[chip // 2, n // per_plane, :, half_lanes(h)], t_ss,
            t_rs.at[chip // 2, n // per_plane, h], (2 * target(z, n) + core, plane),
        )

    def sends_pair(z, n):
        return target(z, n) % 2 != chip % 2

    def sends_sum(z, n):
        return (target(z, n) % 2 == chip % 2) & (target(z, n) != chip)

    def multiply(lhs, rhs):
        return lax.dot_general(lhs, rhs, (((0,), (0,)), ((), ())), preferred_element_type=F32).astype(BF16)

    def add(x, y):
        return (x.astype(F32) + y.astype(F32)).astype(BF16)

    def compute(s):
        own, far, comes, wide, z, n, f, h = decode(s)

        @pl.when(comes)
        def _():
            arrive(z, n)

            @pl.when(wide)
            def _():
                arrive(z, n + 1)

        def both():
            return jnp.concatenate([gathered[z, n], gathered[z, n + 1]], axis=1)

        @pl.when(own & wide)
        def _():
            part = multiply(both(), kept[...])
            work[z, n] = part[:LANES]
            work[z, n + 1] = part[LANES:]

        @pl.when(own & jnp.logical_not(wide))
        def _():
            work[z, n] = multiply(gathered[z, n], kept[...])

        @pl.when(far & wide)
        def _():
            @pl.when((f == 0) & (n == 0))
            def _():
                for i in range(per_half):
                    kept_copy_in(h, i).wait_recv()

            part = multiply(both(), kept_end[h])
            work_far[f, n, h] = part[:LANES]
            work_far[f, n + 1, h] = part[LANES:]

        @pl.when(far & jnp.logical_not(wide))
        def _():
            for i in range(HALVES):
                work_far[f, n, i] = multiply(gathered[z, n], kept_end[i])

        there, n_other = other(wide, n)

        @pl.when(own & there)
        def _():
            core_copy(z, n_other).start()

        @pl.when(far & there & wide)
        def _():
            far_core_copy(f, n_other, h).start()

        @pl.when(far & there & jnp.logical_not(wide))
        def _():
            for i in range(HALVES):
                far_core_copy(f, n_other, i).start()

    def join_far(f, z, n, h):
        far_core_copy(f, n, h).wait_recv()
        work_far[f, n, h] = add(work_far[f, n, h], core_far[f, n // 2, h])
        far_copy(f, z, n, h, near_end).start()

    def join_cores(s):
        own, far, comes, wide, z, n, f, h = decode(s)
        here, n = mine(wide, n)

        @pl.when(own & here)
        def _():
            core_copy(z, n).wait_recv()
            work[z, n] = add(work[z, n], core_in[z, n // 2])

            @pl.when(sends_pair(z, n))
            def _():
                for i in range(HALVES):
                    pair_copy(z, n, i).start()

        @pl.when(far & here & wide)
        def _():
            join_far(f, z, n, h)

        @pl.when(far & here & jnp.logical_not(wide))
        def _():
            for i in range(HALVES):
                join_far(f, z, n, i)

    def join_chips(s, carry):
        own, far, comes, wide, z, n, f, h = decode(s)
        here, n = mine(wide, n)

        @pl.when(own & here & sends_sum(z, n))
        def _():
            for i in range(HALVES):
                pair_copy(z, n, i).wait_recv()
                lanes = pl.ds(i * half_width, half_width)
                work[z, n, :, lanes] = add(work[z, n, :, lanes], pair[z, n // 2, :, lanes])
                target_copy(z, n, i).start()

        return carry

    def joined(s):
        return jnp.clip(jnp.minimum(2 * (s - three + 1), s - LAG), 0, steps)

    def step_body(s, carry):
        compute(s)
        join_cores(s - JOIN)
        lax.fori_loop(joined(s - 1), joined(s), join_chips, 0)
        return carry

    lax.fori_loop(0, steps + JOIN, step_body, 0)
    lax.fori_loop(joined(steps + JOIN - 1), steps, join_chips, 0)

    n_pass = n_far * n_chunk * HALVES

    def passed(e):
        v = e % ((n_far - 1) * n_chunk)
        w = e - (n_far - 1) * n_chunk * HALVES
        f = jnp.where(w < 0, v // n_chunk, n_far - 1)
        n = jnp.where(w < 0, v % n_chunk, w // HALVES)
        h = jnp.where(w < 0, e // ((n_far - 1) * n_chunk), w % HALVES)
        return f, far_plane(f), n, h

    @pl.when(is_end)
    def _():
        def pass_on(e, carry):
            @pl.when(e < n_pass)
            def _():
                f, z, n, h = passed(e)

                @pl.when(n % 2 == core)
                def _():
                    far_copy(f, z, n, h, plane).wait_recv()

                    @pl.when(sends_pair(z, n))
                    def _():
                        pair_copy(z, n, h).start()

            @pl.when(e >= PASS_LAG)
            def _():
                f, z, n, h = passed(e - PASS_LAG)

                @pl.when((n % 2 == core) & sends_sum(z, n))
                def _():
                    pair_copy(z, n, h).wait_recv()
                    lanes = half_lanes(h)
                    work[z, n, :, lanes] = add(work[z, n, :, lanes], pair[z, n // 2, :, lanes])
                    target_copy(z, n, h).start()

            return carry

        lax.fori_loop(0, n_pass + PASS_LAG, pass_on, 0)

    own_z, own_b = me // per_plane, me % per_plane
    for kb in range(n_kb):
        n = kb * per_plane + own_b
        for h in range(HALVES):
            pair_copy(own_z, n, h).wait_recv()
        total = work[own_z, n].astype(F32) + pair[own_z, n // 2].astype(F32)
        for step in range(1, n_chip // 2):
            source = (chip // 2 + step) % (n_chip // 2)
            for h in range(HALVES):
                remote(
                    work.at[own_z, n, :, half_lanes(h)], sums.at[source, kb, :, half_lanes(h)], t_ss,
                    t_rs.at[source, kb, h], (2 * (2 * source + chip % 2) + core, plane),
                ).wait_recv()
            total += sums[source, kb].astype(F32)
        out[kb * LANES : (kb + 1) * LANES, :] = total.astype(BF16)

    def drain_blocks(step, carry):
        for q in range(PIECES):
            a_copy(q, (me + step) % n_row).wait_send()
        return carry

    lax.fori_loop(1, n_row, drain_blocks, 0)

    def sent(ref, sem):
        remote(ref, ref, sem, sem, (partner, plane)).wait_send()

    sent(pair.at[: n_col // 2], p_ss)
    if n_chip > 2:
        sent(sums.at[: n_chip // 2 - 1], t_ss)

    @pl.when(is_end)
    def _():
        sent(core_in.at[:2], c_ss)
        for q in range(PIECES):
            kept_copy(q).wait_send()

    @pl.when(jnp.logical_not(is_end))
    def _():
        sent(core_in, c_ss)

    @pl.when(is_helper)
    def _():
        sent(core_far, d_ss)
        sent(core_far, f_ss)

    def drain_gathered(z, carry):
        @pl.when(goes_right(z))
        def _():
            sent(gathered.at[z], r_ss.at[z])

        @pl.when(goes_left(z))
        def _():
            sent(gathered.at[z], l_ss.at[z])

        return carry

    lax.fori_loop(0, n_col, drain_gathered, 0)


def body(integrals, coeffs, mask, offsets, atom_of_slot):
    n_row = lax.axis_size("row")
    n_col = lax.axis_size("col")
    me = lax.axis_index("row")
    per_dev, atom_w, row_width = integrals.shape
    rows, cols = coeffs.shape
    cap = max(2, -(-per_dev // n_row))
    slots = n_row * cap
    block = cols * n_col // n_row
    n_chunk = cols // LANES
    n_kb = block // LANES

    n_atom = atom_of_slot.shape[0]

    slot = jnp.arange(n_atom, dtype=jnp.int32)
    local = lax.optimization_barrier(atom_of_slot - me * per_dev)
    owner = (local + me * per_dev) // per_dev
    holder = slot // per_dev
    flow = holder * n_row + owner
    rank = jnp.sum(((flow[None, :] == flow[:, None]) & (slot[None, :] < slot[:, None])).astype(jnp.int32), axis=1)
    goes = jnp.where(holder == me, owner * cap + rank, -1)
    comes = local + slots
    entry = jnp.arange(slots + per_dev, dtype=jnp.int32)[:, None]
    meta = jnp.sum(
        jnp.where(
            entry < slots,
            jnp.where(goes[None, :] == entry, (slot - me * per_dev)[None, :], 0),
            jnp.where(comes[None, :] == entry, (holder * cap + rank)[None, :], 0),
        ),
        axis=1,
    )

    packed = rows * 3 // 4
    dma = pltpu.SemaphoreType.DMA
    n_chip = n_row // 2
    n_far = n_col - 2
    narrow = row_width // HALVES
    moved = [pltpu.VMEM((n_row, cap, atom_w, row_width // PIECES), BF16)] * (2 * PIECES)
    smem = pl.BlockSpec(memory_space=pltpu.SMEM)
    vmem = pl.BlockSpec(memory_space=pltpu.VMEM)
    return pl.pallas_call(
        functools.partial(kernel, n_row, n_col, cap, n_chunk),
        out_shape=jax.ShapeDtypeStruct((block, row_width), BF16),
        in_specs=[smem, smem, smem, vmem, vmem],
        out_specs=vmem,
        scratch_shapes=moved
        + [
            pltpu.VMEM((packed, row_width), BF16),
            pltpu.VMEM((HALVES, packed, narrow), BF16),
            pltpu.VMEM((n_col, n_chunk, packed, LANES), BF16),
            pltpu.VMEM((n_col, n_chunk, LANES, row_width), BF16),
            pltpu.VMEM((n_col, n_chunk // 2, LANES, row_width), BF16),
            pltpu.VMEM((n_far, n_chunk, HALVES, LANES, narrow), BF16),
            pltpu.VMEM((n_far, n_chunk // 2, HALVES, LANES, narrow), BF16),
            pltpu.VMEM((n_col, n_chunk // 2, LANES, row_width), BF16),
            pltpu.VMEM((n_chip // 2, n_kb, LANES, row_width), BF16),
            dma((PIECES, n_row)),
            dma((PIECES, n_row)),
            dma((n_col,)),
            dma((n_col,)),
            dma((n_col, n_chunk, PARTS)),
            dma,
            dma((n_col, n_chunk // 2)),
            dma,
            dma((n_far, n_chunk // 2, HALVES)),
            dma,
            dma((n_col, n_chunk // 2, HALVES)),
            dma,
            dma((n_chip // 2, n_kb, HALVES)),
            dma,
            dma((n_far, n_chunk, HALVES)),
            dma((PIECES,)),
            dma((PIECES,)),
        ],
        compiler_params=pltpu.CompilerParams(
            collective_id=0, has_side_effects=True, vmem_limit_bytes=62 << 20
        ),
    )(meta, offsets, mask.T, integrals, coeffs)


def solution(mesh):
    in_specs = (P("row", None, "col"), P("row", "col"), P(), P(), P())
    out_specs = P("row", "col")
    return jax.shard_map(body, mesh=mesh, in_specs=in_specs, out_specs=out_specs, check_vma=False)
```
